16 devices in a mesh: dp: 2 (over z), ep: 8 (over y, x, core).
Axes of the slice: x: 2, y: 2, z: 2, core: 2. Of those that a mesh axis runs over, the one named last changes fastest.
Arguments:
- x_in: bfloat16 [8192, 4096], P(('dp', 'ep'))
- ln_gain: float32 [4096], replicated
- ln_bias: float32 [4096], replicated
- w_router: bfloat16 [4096, 16], replicated
- w_gate: bfloat16 [16, 4096, 960], P('ep')
- w_up: bfloat16 [16, 4096, 960], P('ep')
- w_down: bfloat16 [16, 960, 4096], P('ep')
- expert_ids: int32 [8192, 2], P(('dp', 'ep'))
- slot_ids: int32 [8192, 2], P(('dp', 'ep'))
- d_out: bfloat16 [8192, 4096], P(('dp', 'ep'))
Outputs:
- output 1: bfloat16 [8192, 4096], P(('dp', 'ep'))
- output 2: bfloat16 [8192, 4096], P(('dp', 'ep'))
- output 3: float32 [4096], replicated
- output 4: float32 [4096], replicated
- output 5: float32 [4096, 16], replicated
- output 6: float32 [16, 4096, 960], P('ep')
- output 7: float32 [16, 4096, 960], P('ep')
- output 8: float32 [16, 960, 4096], P('ep')
All inputs are finite; a program needn't handle non-finite values.
Results may differ from the reference program's by a relative error of at most 0.00544038.
Values are sent between devices in bfloat16 or wider.
A program may use at most 1 GiB of HBM per device.

```python
import jax
import jax.numpy as jnp
from jax import lax

D = 4096
FF = 960
EXPERTS = 16
TOP = 2
TOKENS_DEV = 512
DEVICES = 16
CAPACITY = 80
TOKENS = DEVICES * TOKENS_DEV
SLOT_ROWS = EXPERTS * CAPACITY
LN_EPS = 1e-5


def draw_routing(key_route):
    key_hot, key_perm, key_first, key_shift = jax.random.split(key_route, 4)
    hot_expert = jax.random.randint(key_hot, (DEVICES, 1), 0, EXPERTS)
    perm_keys = jax.random.split(key_perm, DEVICES)
    perm_pos = jax.vmap(lambda key_one: jax.random.permutation(key_one, TOKENS_DEV))(perm_keys)
    forced = perm_pos < (3 * CAPACITY) // 2
    first_pick = jax.random.randint(key_first, (DEVICES, TOKENS_DEV), 0, EXPERTS)
    first_pick = jnp.where(forced, hot_expert, first_pick)
    shift_by = jax.random.randint(key_shift, (DEVICES, TOKENS_DEV), 1, EXPERTS)
    second_pick = (first_pick + shift_by) % EXPERTS
    choice = jnp.stack([first_pick, second_pick], axis=-1)
    flat_pick = choice.reshape(DEVICES, TOKENS_DEV * TOP)
    onehot = (flat_pick[:, :, None] == jnp.arange(EXPERTS)[None, None, :]).astype(jnp.int32)
    before = jnp.cumsum(onehot, axis=1) - onehot
    pair_rank = jnp.sum(before * onehot, axis=-1)
    slot_pos = jnp.where(pair_rank < CAPACITY, pair_rank, -1)
    return choice.reshape(TOKENS, TOP).astype(jnp.int32), slot_pos.reshape(TOKENS, TOP).astype(jnp.int32)


def setup_inputs(seed: int = 0) -> dict:
    key_root = jax.random.key(seed)
    key_list = jax.random.split(key_root, 10)
    x_in = jax.random.normal(key_list[0], (TOKENS, D), jnp.float32).astype(jnp.bfloat16)
    ln_gain = 1.0 + 0.3 * jax.random.normal(key_list[1], (D,), jnp.float32)
    ln_bias = 0.3 * jax.random.normal(key_list[2], (D,), jnp.float32)
    w_router = (jax.random.normal(key_list[3], (D, EXPERTS), jnp.float32) * D ** -0.5).astype(jnp.bfloat16)
    w_gate = (jax.random.normal(key_list[4], (EXPERTS, D, FF), jnp.float32) * D ** -0.5).astype(jnp.bfloat16)
    w_up = (jax.random.normal(key_list[5], (EXPERTS, D, FF), jnp.float32) * D ** -0.5).astype(jnp.bfloat16)
    w_down = (jax.random.normal(key_list[6], (EXPERTS, FF, D), jnp.float32) * (2.0 * FF ** -0.5)).astype(jnp.bfloat16)
    expert_ids, slot_ids = draw_routing(key_list[7])
    d_out = jax.random.normal(key_list[8], (TOKENS, D), jnp.float32).astype(jnp.bfloat16)
    return {"x_in": x_in, "ln_gain": ln_gain, "ln_bias": ln_bias, "w_router": w_router, "w_gate": w_gate, "w_up": w_up, "w_down": w_down, "expert_ids": expert_ids, "slot_ids": slot_ids, "d_out": d_out}


def to_bf16_grid(array_in):
    return array_in.astype(jnp.bfloat16).astype(jnp.float32)


def reference(x_in, ln_gain, ln_bias, w_router, w_gate, w_up, w_down, expert_ids, slot_ids, d_out):
    ids_dev = expert_ids.reshape(DEVICES, TOKENS_DEV, TOP)
    slots_dev = slot_ids.reshape(DEVICES, TOKENS_DEV, TOP)
    target = jnp.where(slots_dev >= 0, ids_dev * CAPACITY + slots_dev, -1)
    pair_hot = (target[..., None] == jnp.arange(SLOT_ROWS)).astype(jnp.float32)
    token_hot = jnp.sum(pair_hot, axis=2)

    def block_fn(x_f, gain_vec, bias_vec, router_f, gate_f, up_f, down_f):
        x_dev = x_f.reshape(DEVICES, TOKENS_DEV, D)
        mean_x = jnp.mean(x_dev, axis=-1, keepdims=True)
        centered = x_dev - mean_x
        var_x = jnp.mean(centered * centered, axis=-1, keepdims=True)
        normed = centered * lax.rsqrt(var_x + LN_EPS)
        hidden = to_bf16_grid(normed * gain_vec + bias_vec)
        logits = jnp.einsum("dtm,me->dte", hidden, router_f)
        gate_probs = jax.nn.softmax(jnp.take_along_axis(logits, ids_dev, axis=-1), axis=-1)
        buffers = to_bf16_grid(jnp.einsum("dts,dtm->dsm", token_hot, hidden))
        buffers = buffers.reshape(DEVICES, EXPERTS, CAPACITY, D)
        act_gate = to_bf16_grid(jnp.einsum("decm,emf->decf", buffers, gate_f))
        act_up = to_bf16_grid(jnp.einsum("decm,emf->decf", buffers, up_f))
        act_mix = to_bf16_grid(jax.nn.silu(act_gate) * act_up)
        expert_out = to_bf16_grid(jnp.einsum("decf,efm->decm", act_mix, down_f))
        pair_out = jnp.einsum("dtks,dsm->dtkm", pair_hot, expert_out.reshape(DEVICES, SLOT_ROWS, D))
        mixed = jnp.einsum("dtk,dtkm->dtm", gate_probs, pair_out)
        return to_bf16_grid(x_dev + mixed).reshape(TOKENS, D)

    moe_f, pullback = jax.vjp(block_fn, x_in.astype(jnp.float32), ln_gain, ln_bias, w_router.astype(jnp.float32), w_gate.astype(jnp.float32), w_up.astype(jnp.float32), w_down.astype(jnp.float32))
    grad_list = pullback(d_out.astype(jnp.float32))
    return (moe_f.astype(jnp.bfloat16), grad_list[0].astype(jnp.bfloat16), grad_list[1], grad_list[2], grad_list[3], grad_list[4], grad_list[5], grad_list[6])
```

```python
import jax
import jax.numpy as jnp
from jax import lax
from jax.experimental import pallas as pl
from jax.experimental.pallas import tpu as pltpu
from jax.sharding import PartitionSpec as P


LN_EPS = 1e-5
SWAP = [(0, 1), (1, 0)]


def capacity_for(tokens_dev, experts, n_top):
    return 8 * ((5 * tokens_dev * n_top + 32 * experts - 1) // (32 * experts))


def norm_forward(x_loc, ln_gain, ln_bias):
    x_f = x_loc.astype(jnp.float32)
    mean_x = jnp.mean(x_f, axis=-1, keepdims=True)
    centered = x_f - mean_x
    var_x = jnp.mean(centered * centered, axis=-1, keepdims=True)
    inv_std = lax.rsqrt(var_x + LN_EPS)
    normed = centered * inv_std
    hidden = (normed * ln_gain + ln_bias).astype(jnp.bfloat16)
    return x_f, hidden, normed, inv_std


def norm_backward(d_hidden, normed, inv_std, ln_gain):
    d_normed = d_hidden * ln_gain
    mean_dn = jnp.mean(d_normed, axis=-1, keepdims=True)
    mean_dnn = jnp.mean(d_normed * normed, axis=-1, keepdims=True)
    return inv_std * (d_normed - mean_dn - normed * mean_dnn)


def dot32(lhs, rhs, dims):
    return lax.dot_general(lhs, rhs, (dims, ((), ())), preferred_element_type=jnp.float32)


def acts(rows, gate_e, up_e):
    pre_gate = dot32(rows, gate_e, ((1,), (0,))).astype(jnp.bfloat16)
    pre_up = dot32(rows, up_e, ((1,), (0,))).astype(jnp.bfloat16)
    gate_f = pre_gate.astype(jnp.float32)
    act_mix = (gate_f * jax.nn.sigmoid(gate_f) * pre_up.astype(jnp.float32)).astype(jnp.bfloat16)
    return pre_gate, pre_up, act_mix


def act_grads(pre_gate, pre_up, grad_rows, down_e):
    d_mix = dot32(grad_rows, down_e, ((1,), (1,))).astype(jnp.bfloat16).astype(jnp.float32)
    gate_f = pre_gate.astype(jnp.float32)
    sig_gate = jax.nn.sigmoid(gate_f)
    up_f = pre_up.astype(jnp.float32)
    d_pre_gate = (d_mix * up_f * sig_gate * (1.0 + gate_f * (1.0 - sig_gate))).astype(jnp.bfloat16)
    d_pre_up = (d_mix * gate_f * sig_gate).astype(jnp.bfloat16)
    return d_pre_gate, d_pre_up


def row_sum_dot(lhs_a, rhs_a, lhs_b, rhs_b):
    dims = (((0,), (0,)), ((), ()))
    part = lax.dot_general(lhs_a, rhs_a, dims, preferred_element_type=jnp.float32)
    return part + lax.dot_general(lhs_b, rhs_b, dims, preferred_element_type=jnp.float32)


def weight_grad(expert, experts, cols_a, cols_b, rows_a, rows_b, prev, tile=512):
    n_rows, width = rows_a.shape
    inner = cols_a.shape[1]

    def body(*refs):
        ca, cb, ra, rb = refs[:4]
        refs[-1][0] = row_sum_dot(ca[...], ra[...], cb[...], rb[...])

    row_spec = pl.BlockSpec((n_rows, tile), lambda i: (0, i))
    full_spec = pl.BlockSpec((n_rows, inner), lambda i: (0, 0))
    return pl.pallas_call(
        body,
        grid=(width // tile,),
        in_specs=[full_spec, full_spec, row_spec, row_spec] + [pl.BlockSpec(memory_space=pl.ANY)] * len(prev),
        out_specs=pl.BlockSpec((1, inner, tile), lambda i: (expert, 0, i)),
        out_shape=jax.ShapeDtypeStruct((experts, inner, width), jnp.float32),
        input_output_aliases={4 + i: i for i in range(len(prev))},
        compiler_params=pltpu.CompilerParams(dimension_semantics=("arbitrary",), vmem_limit_bytes=40 * 2**20),
        cost_estimate=pl.CostEstimate(flops=4 * n_rows * width * inner, bytes_accessed=4 * n_rows * width + 4 * width * inner, transcendentals=0),
    )(cols_a, cols_b, rows_a, rows_b, *prev)


def sum_all(mesh_shape, rows):
    n_dp, n_ep = mesh_shape
    n_dev = n_dp * n_ep
    n, width = rows.shape
    cols = width // n_dev

    def body(in_ref, out_ref, got, mine, send_a, recv_a, send_b, recv_b):
        my_dp, my_ep = lax.axis_index("dp"), lax.axis_index("ep")
        me = my_dp * n_ep + my_ep
        barrier = pltpu.get_barrier_semaphore()

        def peer(k):
            other = lax.rem(me + k, n_dev)
            return other, (other // n_ep, lax.rem(other, n_ep))

        for k in range(1, n_dev):
            pl.semaphore_signal(barrier, inc=1, device_id=peer(k)[1], device_id_type=pl.DeviceIdType.MESH)
        pl.semaphore_wait(barrier, n_dev - 1)
        first = []
        for k in range(1, n_dev):
            other, dev = peer(k)
            copy = pltpu.make_async_remote_copy(
                src_ref=in_ref.at[:, pl.ds(pl.multiple_of(other * cols, 128), cols)], dst_ref=got.at[k],
                send_sem=send_a.at[k], recv_sem=recv_a.at[k], device_id=dev, device_id_type=pl.DeviceIdType.MESH)
            copy.start()
            first.append(copy)
        my_cols = pl.ds(pl.multiple_of(me * cols, 128), cols)
        total = in_ref[:, my_cols]
        for k in range(1, n_dev):
            first[k - 1].wait_recv()
            total = total + got[k]
        mine[...] = total
        out_ref[:, my_cols] = total
        for copy in first:
            copy.wait_send()
        second = []
        for k in range(1, n_dev):
            copy = pltpu.make_async_remote_copy(
                src_ref=mine, dst_ref=out_ref.at[:, my_cols],
                send_sem=send_b.at[k], recv_sem=recv_b.at[k], device_id=peer(k)[1], device_id_type=pl.DeviceIdType.MESH)
            copy.start()
            second.append(copy)
        for copy in second:
            copy.wait()

    return pl.pallas_call(
        body,
        in_specs=[pl.BlockSpec(memory_space=pltpu.VMEM)],
        out_specs=pl.BlockSpec(memory_space=pltpu.VMEM),
        out_shape=jax.ShapeDtypeStruct((n, width), jnp.float32),
        scratch_shapes=[pltpu.VMEM((n_dev, n, cols), jnp.float32), pltpu.VMEM((n, cols), jnp.float32)]
        + [pltpu.SemaphoreType.DMA((n_dev,))] * 4,
        compiler_params=pltpu.CompilerParams(collective_id=7, has_side_effects=True),
        name="sum_all",
    )(rows)


def solution(mesh):
    n_ep = mesh.shape["ep"]
    tok_spec = P(("dp", "ep"), None)
    exp_spec = P("ep", None, None)

    def local_step(x_loc, ln_gain, ln_bias, w_router, gate_loc, up_loc, down_loc, ids_loc, slots_loc, dout_loc):
        tokens_dev, model_dim = x_loc.shape
        experts = w_router.shape[1]
        local_exp = gate_loc.shape[0]
        n_top = ids_loc.shape[1]
        capacity = capacity_for(tokens_dev, experts, n_top)
        half = n_ep * capacity
        slot_rows = experts * capacity

        def exchange(rows):
            out = lax.all_to_all(rows.reshape(n_ep, capacity, model_dim), "ep", 0, 0, tiled=True)
            return out.reshape(half, model_dim)

        def swap(rows):
            return lax.ppermute(rows, "dp", SWAP)

        x_f, hidden, normed, inv_std = norm_forward(x_loc, ln_gain, ln_bias)
        pos = (ids_loc % local_exp) * half + (ids_loc // local_exp) * capacity + slots_loc
        pos = jnp.where(slots_loc >= 0, pos, -1)
        row_ids = jnp.arange(slot_rows)
        pair_hit = row_ids[:, None, None] == pos.T[None, :, :]
        row_hot = jnp.any(pair_hit, axis=1).astype(jnp.bfloat16)

        h_own, h_oth, g_own, g_oth = [], [], [], []
        for le in range(local_exp):
            rows = dot32(row_hot[le * half : (le + 1) * half], hidden, ((1,), (0,))).astype(jnp.bfloat16)
            h_own.append(exchange(rows))
            h_oth.append(swap(h_own[le]))

        logits = jnp.dot(hidden, w_router, preferred_element_type=jnp.float32)
        pick_mask = (ids_loc[..., None] == jnp.arange(experts)).astype(jnp.float32)
        gate_probs = jax.nn.softmax(jnp.sum(pick_mask * logits[..., None, :], axis=-1), axis=-1)
        row_prob = jnp.sum(jnp.where(pair_hit, gate_probs.T[None, :, :], 0.0), axis=(1, 2))
        for le in range(local_exp):
            part = slice(le * half, (le + 1) * half)
            rows = (dot32(row_hot[part], dout_loc, ((1,), (0,))) * row_prob[part, None]).astype(jnp.bfloat16)
            g_own.append(exchange(rows))
            g_oth.append(swap(g_own[le]))

        y_ret, d_ret, saved = [], [], []
        for le in range(local_exp):
            pre_gate, pre_up, act_mix = acts(h_own[le], gate_loc[le], up_loc[le])
            y_rows = dot32(act_mix, down_loc[le], ((1,), (0,))).astype(jnp.bfloat16)
            y_ret.append(exchange(y_rows))
            saved.append((pre_gate, pre_up, act_mix))
        own = []
        for le in range(local_exp):
            pre_gate, pre_up, act_mix = saved[le]
            dg, du = act_grads(pre_gate, pre_up, g_own[le], down_loc[le])
            d_rows = (dot32(dg, gate_loc[le], ((1,), (1,))) + dot32(du, up_loc[le], ((1,), (1,)))).astype(jnp.bfloat16)
            d_ret.append(exchange(d_rows))
            own.append((act_mix, dg, du))
        grads = [(), (), ()]
        for le in range(local_exp):
            mix_own, dg_own, du_own = own[le]
            pre_gate, pre_up, mix_oth = acts(h_oth[le], gate_loc[le], up_loc[le])
            dg_oth, du_oth = act_grads(pre_gate, pre_up, g_oth[le], down_loc[le])
            cols = ((dg_own, dg_oth, h_own[le], h_oth[le]), (du_own, du_oth, h_own[le], h_oth[le]), (mix_own, mix_oth, g_own[le], g_oth[le]))
            grads = [weight_grad(le, local_exp, *cols[n], grads[n]) for n in range(3)]
            grads = [(g,) for g in grads]

        ret_rows = jnp.concatenate(y_ret, axis=0)
        pair_hot = (pos[..., None] == row_ids).astype(jnp.bfloat16)
        pair_out = jnp.dot(pair_hot.reshape(tokens_dev * n_top, slot_rows), ret_rows, preferred_element_type=jnp.float32)
        pair_out = pair_out.reshape(tokens_dev, n_top, model_dim)
        moe_out = (x_f + jnp.sum(gate_probs[..., None] * pair_out, axis=1)).astype(jnp.bfloat16)
        dout_f = dout_loc.astype(jnp.float32)
        d_gates = jnp.sum(pair_out * dout_f[:, None, :], axis=-1)
        d_chosen = gate_probs * (d_gates - jnp.sum(gate_probs * d_gates, axis=-1, keepdims=True))
        d_logits = jnp.sum(d_chosen[..., None] * pick_mask, axis=-2)

        d_hidden_moe = dot32(row_hot, jnp.concatenate(d_ret, axis=0), ((0,), (0,)))
        d_hidden_router = jnp.einsum("te,me->tm", d_logits, w_router, preferred_element_type=jnp.float32)
        d_hidden = (d_hidden_moe + d_hidden_router).astype(jnp.bfloat16).astype(jnp.float32)
        grad_x = (dout_f + norm_backward(d_hidden, normed, inv_std, ln_gain)).astype(jnp.bfloat16)
        router_part = dot32(d_logits, hidden.astype(jnp.float32), ((0,), (0,)))
        norm_part = jnp.stack([jnp.sum(d_hidden * normed, axis=0), jnp.sum(d_hidden, axis=0)])
        pad = jnp.zeros((-(experts + 2) % 8, model_dim), jnp.float32)
        sums = sum_all((mesh.shape["dp"], n_ep), jnp.concatenate([router_part, norm_part, pad], axis=0))
        grad_gate, grad_up = (jnp.swapaxes(g[0], 1, 2) for g in grads[:2])
        return moe_out, grad_x, sums[experts], sums[experts + 1], sums[:experts].T, grad_gate, grad_up, grads[2][0]

    return jax.shard_map(local_step, mesh=mesh, in_specs=(tok_spec, P(None), P(None), P(None, None), exp_spec, exp_spec, exp_spec, tok_spec, tok_spec, tok_spec), out_specs=(tok_spec, tok_spec, P(None), P(None), P(None, None), exp_spec, exp_spec, exp_spec), check_vma=False)
```

```python
import jax
import jax.numpy as jnp
from jax import lax
from jax.experimental import pallas as pl
from jax.experimental.pallas import tpu as pltpu
from jax.sharding import PartitionSpec as P


LN_EPS = 1e-5
SWAP = [(0, 1), (1, 0)]


def capacity_for(tokens_dev, experts, n_top):
    return 8 * ((5 * tokens_dev * n_top + 32 * experts - 1) // (32 * experts))


def norm_forward(x_loc, ln_gain, ln_bias):
    x_f = x_loc.astype(jnp.float32)
    mean_x = jnp.mean(x_f, axis=-1, keepdims=True)
    centered = x_f - mean_x
    var_x = jnp.mean(centered * centered, axis=-1, keepdims=True)
    inv_std = lax.rsqrt(var_x + LN_EPS)
    normed = centered * inv_std
    hidden = (normed * ln_gain + ln_bias).astype(jnp.bfloat16)
    return x_f, hidden, normed, inv_std


def norm_backward(d_hidden, normed, inv_std, ln_gain):
    d_normed = d_hidden * ln_gain
    mean_dn = jnp.mean(d_normed, axis=-1, keepdims=True)
    mean_dnn = jnp.mean(d_normed * normed, axis=-1, keepdims=True)
    return inv_std * (d_normed - mean_dn - normed * mean_dnn)


def dot32(lhs, rhs, dims):
    return lax.dot_general(lhs, rhs, (dims, ((), ())), preferred_element_type=jnp.float32)


def row_spec(piece, expert, tile):
    n_src, n_exp, cap, _ = piece.shape
    at = expert if n_exp > 1 else 0
    return pl.BlockSpec((n_src, 1, cap, tile), lambda i: (0, at, 0, i))


def load_rows(refs):
    parts = [ref[...].reshape(ref.shape[0] * ref.shape[2], ref.shape[3]) for ref in refs]
    return parts[0] if len(parts) == 1 else jnp.concatenate(parts, axis=0)


def count_rows(pieces):
    return sum(piece.shape[0] * piece.shape[2] for piece in pieces)


def call(body, flops, moved, **kwargs):
    return pl.pallas_call(
        body,
        compiler_params=pltpu.CompilerParams(dimension_semantics=("arbitrary",), vmem_limit_bytes=48 * 2**20),
        cost_estimate=pl.CostEstimate(flops=flops, bytes_accessed=moved, transcendentals=0),
        **kwargs,
    )


def acts(expert, pieces, gate_t, up_t, tile=1024):
    n_p = len(pieces)
    n_rows = count_rows(pieces)
    _, inner, width = gate_t.shape
    steps = width // tile

    def body(*refs):
        rows = load_rows(refs[:n_p])
        wg, wu, og, ou, om, acc_g, acc_u = refs[n_p:]
        step = pl.program_id(0)
        part_g = dot32(rows, wg[0], ((1,), (1,)))
        part_u = dot32(rows, wu[0], ((1,), (1,)))

        @pl.when(step == 0)
        def _():
            acc_g[...] = part_g
            acc_u[...] = part_u

        @pl.when(step > 0)
        def _():
            acc_g[...] += part_g
            acc_u[...] += part_u

        @pl.when(step == steps - 1)
        def _():
            pre_gate = acc_g[...].astype(jnp.bfloat16)
            pre_up = acc_u[...].astype(jnp.bfloat16)
            og[...] = pre_gate
            ou[...] = pre_up
            gate_f = pre_gate.astype(jnp.float32)
            om[...] = (gate_f * jax.nn.sigmoid(gate_f) * pre_up.astype(jnp.float32)).astype(jnp.bfloat16)

    w_spec = pl.BlockSpec((1, inner, tile), lambda i: (expert, 0, i))
    out = jax.ShapeDtypeStruct((n_rows, inner), jnp.bfloat16)
    return call(
        body, 4 * n_rows * inner * width, 2 * (n_rows + 2 * inner) * width,
        grid=(steps,),
        in_specs=[row_spec(p, expert, tile) for p in pieces] + [w_spec, w_spec],
        out_specs=[pl.BlockSpec((n_rows, inner), lambda i: (0, 0))] * 3,
        out_shape=[out, out, out],
        scratch_shapes=[pltpu.VMEM((n_rows, inner), jnp.float32)] * 2,
    )(*pieces, gate_t, up_t)


def act_grads(expert, pieces, down, pre_gate, pre_up, tile=1024):
    n_p = len(pieces)
    n_rows = count_rows(pieces)
    _, inner, width = down.shape
    steps = width // tile

    def body(*refs):
        rows = load_rows(refs[:n_p])
        wd, ga, ua, odg, odu, acc = refs[n_p:]
        step = pl.program_id(0)
        part = dot32(rows, wd[0], ((1,), (1,)))

        @pl.when(step == 0)
        def _():
            acc[...] = part

        @pl.when(step > 0)
        def _():
            acc[...] += part

        @pl.when(step == steps - 1)
        def _():
            d_mix = acc[...].astype(jnp.bfloat16).astype(jnp.float32)
            gate_f = ga[...].astype(jnp.float32)
            up_f = ua[...].astype(jnp.float32)
            sig_gate = jax.nn.sigmoid(gate_f)
            odg[...] = (d_mix * up_f * sig_gate * (1.0 + gate_f * (1.0 - sig_gate))).astype(jnp.bfloat16)
            odu[...] = (d_mix * gate_f * sig_gate).astype(jnp.bfloat16)

    full = pl.BlockSpec((n_rows, inner), lambda i: (0, 0))
    out = jax.ShapeDtypeStruct((n_rows, inner), jnp.bfloat16)
    return call(
        body, 2 * n_rows * inner * width, 2 * (n_rows + inner) * width,
        grid=(steps,),
        in_specs=[row_spec(p, expert, tile) for p in pieces] + [pl.BlockSpec((1, inner, tile), lambda i: (expert, 0, i)), full, full],
        out_specs=[full, full],
        out_shape=[out, out],
        scratch_shapes=[pltpu.VMEM((n_rows, inner), jnp.float32)],
    )(*pieces, down, pre_gate, pre_up)


def project(expert, cols, weights, prev, shape, tile=512):
    n_c = len(cols)
    n_src, _, cap, width = shape
    n_rows, inner = cols[0].shape

    def body(*refs):
        total = dot32(refs[0][...], refs[n_c][0], ((1,), (0,)))
        for n in range(1, n_c):
            total = total + dot32(refs[n][...], refs[n_c + n][0], ((1,), (0,)))
        refs[-1][...] = total.astype(jnp.bfloat16).reshape(n_src, 1, cap, tile)

    return call(
        body, 2 * n_c * n_rows * inner * width, 2 * (n_rows + n_c * inner) * width,
        grid=(width // tile,),
        in_specs=[pl.BlockSpec((n_rows, inner), lambda i: (0, 0))] * n_c
        + [pl.BlockSpec((1, inner, tile), lambda i: (expert, 0, i))] * n_c
        + [pl.BlockSpec(memory_space=pl.ANY)] * len(prev),
        out_specs=pl.BlockSpec((n_src, 1, cap, tile), lambda i: (0, expert, 0, i)),
        out_shape=jax.ShapeDtypeStruct(shape, jnp.bfloat16),
        input_output_aliases={2 * n_c + n: n for n in range(len(prev))},
    )(*cols, *weights, *prev)


def weight_grads(expert, experts, terms, prev, tile=512):
    row_sets, cols, which = [], [], []
    for cols_a, cols_b, pieces_a, pieces_b in terms:
        pieces = list(pieces_a) + list(pieces_b)
        found = [n for n, other in enumerate(row_sets) if all(p is q for p, q in zip(other, pieces))]
        if not found:
            row_sets.append(pieces)
        which.append(found[0] if found else len(row_sets) - 1)
        cols += [cols_a, cols_b]
    n_t = len(terms)
    flat = [p for pieces in row_sets for p in pieces]
    n_a, inner = cols[0].shape
    n_rows = count_rows(row_sets[0])
    width = flat[0].shape[3]
    n_in = len(cols) + len(flat) + len(prev)

    def body(*refs):
        outs = refs[n_in : n_in + n_t]
        turned = refs[n_in + n_t :]

        @pl.when(pl.program_id(0) == 0)
        def _():
            for n in range(n_t):
                turned[n][:, :n_a] = refs[2 * n][...].T
                turned[n][:, n_a:] = refs[2 * n + 1][...].T

        at = len(cols)
        rows = []
        for pieces in row_sets:
            rows.append(load_rows(refs[at : at + len(pieces)]))
            at += len(pieces)
        for n in range(n_t):
            outs[n][0] = dot32(turned[n][...], rows[which[n]], ((1,), (0,)))

    full = [pl.BlockSpec(c.shape, lambda i: (0, 0)) for c in cols]
    return call(
        body, 2 * n_t * n_rows * inner * width, 2 * len(row_sets) * n_rows * width + 4 * n_t * inner * width,
        grid=(width // tile,),
        in_specs=full + [row_spec(p, expert, tile) for p in flat] + [pl.BlockSpec(memory_space=pl.ANY)] * len(prev),
        out_specs=[pl.BlockSpec((1, inner, tile), lambda i: (expert, 0, i))] * n_t,
        out_shape=[jax.ShapeDtypeStruct((experts, inner, width), jnp.float32)] * n_t,
        scratch_shapes=[pltpu.VMEM((inner, n_rows), jnp.bfloat16)] * n_t,
        input_output_aliases={len(cols) + len(flat) + n: n for n in range(len(prev))},
    )(*cols, *flat, *prev)


def solution(mesh):
    n_dp, n_ep = mesh.shape["dp"], mesh.shape["ep"]
    tok_spec = P(("dp", "ep"), None)
    exp_spec = P("ep", None, None)

    def local_step(x_loc, ln_gain, ln_bias, w_router, gate_loc, up_loc, down_loc, ids_loc, slots_loc, dout_loc):
        tokens_dev, model_dim = x_loc.shape
        experts = w_router.shape[1]
        local_exp = gate_loc.shape[0]
        n_top = ids_loc.shape[1]
        capacity = capacity_for(tokens_dev, experts, n_top)
        slot_rows = experts * capacity
        shape = (n_ep, local_exp, capacity, model_dim)
        gate_t, up_t = jnp.swapaxes(gate_loc, 1, 2), jnp.swapaxes(up_loc, 1, 2)
        me = lax.axis_index("ep")
        chip = me // 2

        def exchange(rows):
            return lax.all_to_all(rows, "ep", 0, 0, tiled=True)

        def swap(rows):
            return lax.ppermute(rows, "dp", SWAP)

        def near_pieces(rows):
            mine = lax.dynamic_slice_in_dim(rows, me, 1, 0)
            other = lax.dynamic_slice_in_dim(rows, me + 1 - 2 * (me % 2), 1, 0)
            cross = [(i * n_ep + j, (1 - i) * n_ep + (j ^ 1)) for i in range(n_dp) for j in range(n_ep)]
            other = lax.ppermute(other, ("dp", "ep"), cross)
            return [swap(mine), other]

        def far_pieces(rows, expert=None):
            first, n_exp = (0, local_exp) if expert is None else (expert, 1)
            out = []
            for d in range(1, n_ep // 2):
                start = 2 * jnp.bitwise_xor(chip, d)
                part = lax.dynamic_slice(rows, (start, first, 0, 0), (2, n_exp, capacity, model_dim))
                out.append(swap(part))
            return out

        def sum_all(part, stages):
            def flip(e, d):
                pairs = [(i * n_ep + j, (i ^ d) * n_ep + (j ^ e)) for i in range(n_dp) for j in range(n_ep)]
                return lax.ppermute(part, ("dp", "ep"), pairs)

            for bits in stages:
                got = [flip(*bit) for bit in bits]
                if len(bits) == 2:
                    got.append(flip(bits[0][0] ^ bits[1][0], bits[0][1] ^ bits[1][1]))
                part = part + got[0] if len(bits) == 1 else (part + got[0]) + (got[1] + got[2])
            return part

        bit_core, bit_x, bit_y, bit_z = (1, 0), (2, 0), (4, 0), (0, 1)
        x_f, hidden, normed, inv_std = norm_forward(x_loc, ln_gain, ln_bias)
        pos = jnp.where(slots_loc >= 0, ids_loc * capacity + slots_loc, -1)
        row_ids = jnp.arange(slot_rows)
        pair_hit = row_ids[:, None, None] == pos.T[None, :, :]
        row_hot = jnp.any(pair_hit, axis=1).astype(jnp.bfloat16)
        send_h = dot32(row_hot, hidden, ((1,), (0,))).astype(jnp.bfloat16).reshape(shape)
        h_near = near_pieces(send_h)
        h_own = [exchange(send_h)]
        h_oth = h_near + far_pieces(h_own[0])

        logits = jnp.dot(hidden, w_router, preferred_element_type=jnp.float32)
        pick_mask = (ids_loc[..., None] == jnp.arange(experts)).astype(jnp.float32)
        gate_probs = jax.nn.softmax(jnp.sum(pick_mask * logits[..., None, :], axis=-1), axis=-1)
        row_prob = jnp.sum(jnp.where(pair_hit, gate_probs.T[None, :, :], 0.0), axis=(1, 2))
        send_g = (dot32(row_hot, dout_loc, ((1,), (0,))) * row_prob[:, None]).astype(jnp.bfloat16).reshape(shape)
        g_near = near_pieces(send_g)
        g_own = [exchange(send_g)]
        g_oth = [g_near + far_pieces(g_own[0], le) for le in range(local_exp)]

        saved, y_rows = [], ()
        for le in range(local_exp):
            saved.append(acts(le, h_own, gate_t, up_t))
            y_rows = (project(le, [saved[le][2]], [down_loc], y_rows, shape),)
        y_ret = exchange(y_rows[0])
        own, d_rows = [], ()
        for le in range(local_exp):
            pre_gate, pre_up, act_mix = saved[le]
            dg, du = act_grads(le, g_own, down_loc, pre_gate, pre_up)
            d_rows = (project(le, [dg, du], [gate_t, up_t], d_rows, shape),)
            own.append((act_mix, dg, du))
        d_ret = exchange(d_rows[0])
        grads = []
        oth_acts = [acts(le, h_oth, gate_t, up_t) for le in range(local_exp)]
        for le in range(local_exp):
            pre_gate, pre_up, mix_oth = oth_acts[le]
            dg_oth, du_oth = act_grads(le, g_oth[le], down_loc, pre_gate, pre_up)
            mix_own, dg_own, du_own = own[le]
            terms = [(dg_own, dg_oth, h_own, h_oth), (du_own, du_oth, h_own, h_oth), (mix_own, mix_oth, g_own, g_oth[le])]
            if le + 1 < local_exp:
                grads = weight_grads(le, local_exp, terms, grads)
            else:
                grads = weight_grads(le, local_exp, terms[:2], grads[:2]) + weight_grads(le, local_exp, terms[2:], grads[2:])

        ret_rows = y_ret.reshape(slot_rows, model_dim)
        pair_hot = (pos[..., None] == row_ids).astype(jnp.bfloat16)
        pair_out = jnp.dot(pair_hot.reshape(tokens_dev * n_top, slot_rows), ret_rows, preferred_element_type=jnp.float32)
        pair_out = pair_out.reshape(tokens_dev, n_top, model_dim)
        moe_out = (x_f + jnp.sum(gate_probs[..., None] * pair_out, axis=1)).astype(jnp.bfloat16)
        dout_f = dout_loc.astype(jnp.float32)
        d_gates = jnp.sum(pair_out * dout_f[:, None, :], axis=-1)
        moe_out, d_gates = lax.optimization_barrier((moe_out, d_gates))
        d_chosen = gate_probs * (d_gates - jnp.sum(gate_probs * d_gates, axis=-1, keepdims=True))
        d_logits = jnp.sum(d_chosen[..., None] * pick_mask, axis=-2)
        high = lax.Precision.HIGHEST
        router_part = lax.dot_general(d_logits, hidden.astype(jnp.float32), (((0,), (0,)), ((), ())), precision=high)
        router_grad = sum_all(router_part, [[bit_core], [bit_x, bit_y], [bit_z]])

        d_hidden_moe = dot32(row_hot, d_ret.reshape(slot_rows, model_dim), ((0,), (0,)))
        d_hidden_router = jnp.einsum("te,me->tm", d_logits, w_router.astype(jnp.float32), precision=high)
        d_hidden = (d_hidden_moe + d_hidden_router).astype(jnp.bfloat16).astype(jnp.float32)
        grad_x = (dout_f + norm_backward(d_hidden, normed, inv_std, ln_gain)).astype(jnp.bfloat16)
        norm_part = jnp.stack([jnp.sum(d_hidden * normed, axis=0), jnp.sum(d_hidden, axis=0)])
        norm_grads = sum_all(norm_part, [[bit_core, bit_x], [bit_y, bit_z]])
        grad_gate, grad_up = (jnp.swapaxes(g, 1, 2) for g in grads[:2])
        return moe_out, grad_x, norm_grads[0], norm_grads[1], router_grad.T, grad_gate, grad_up, grads[2]

    return jax.shard_map(local_step, mesh=mesh, in_specs=(tok_spec, P(None), P(None), P(None, None), exp_spec, exp_spec, exp_spec, tok_spec, tok_spec, tok_spec), out_specs=(tok_spec, tok_spec, P(None), P(None), P(None, None), exp_spec, exp_spec, exp_spec), check_vma=False)
```
